256 devices in a mesh: row: 32 (over y, z), col: 8 (over x, core).
Axes of the slice: x: 4, y: 4, z: 8, core: 2. Of those that a mesh axis runs over, the one named last changes fastest.
Arguments:
- layer_input: bfloat16 [8192, 8192], P('row'), may hold values from -7 to 7
- gain: float32 [8192], replicated, may hold values from 0.5 to 6
- d_query: bfloat16 [8192, 4096], P('row', 'col'), may hold values from -6 to 6
- d_keyval: bfloat16 [8192, 2048], P('row', 'col'), may hold values from -6 to 6
- w_query: bfloat16 [8192, 4096], P('row', 'col'), may hold values from -0.0625 to 0.0625
- w_keyval: bfloat16 [8192, 2048], P('row', 'col'), may hold values from -1 to 1
- d_resid: bfloat16 [8192, 8192], P('row', 'col'), may hold values from -6 to 6
Outputs:
- d_input: bfloat16 [8192, 8192], P('row', 'col')
- grad_wq: bfloat16 [8192, 4096], P('row', 'col')
- grad_wkv: bfloat16 [8192, 2048], P('row', 'col')
- grad_gain: float32 [8192], P('col')
- grad_square_sum: float32 [], replicated
The draws below stay inside these ranges and needn't reach their ends.
All inputs are finite; a program needn't handle non-finite values.
Results may differ from the reference program's by a relative error of at most 0.023.
Values may be sent and summed in bfloat16 or wider, within the bound.
No kernel may reach another device: no remote copies, remote signals or barrier semaphores. Data moves between devices by JAX's collectives and lax.ppermute only.
A program may use at most 128 MiB of HBM per device.

```python
import jax
import jax.numpy as jnp
from jax import lax

D = 8192
TOK_DEV = 256
QW = 4096
KVW = 2048
TOKENS = 8192
N_ROW = 32
N_COL = 8


def input_values(key):
    input_key = jax.random.fold_in(key, 101)
    return jnp.clip(jax.random.normal(input_key, (TOKENS, D), jnp.float32), -6.0, 6.0)


def keyval_values(key):
    weight_key = jax.random.fold_in(key, 202)
    factor = jnp.float32(1.0) / jnp.sqrt(jnp.float32(D))
    return jnp.clip(jax.random.normal(weight_key, (D, KVW), jnp.float32), -6.0, 6.0) * factor


def draw_layer_input(key, part):
    return input_values(key).astype(jnp.bfloat16)


def draw_gain(key, part):
    gain_key = jax.random.fold_in(key, 404)
    position = jnp.arange(D, dtype=jnp.float32) / jnp.float32(max(D - 1, 1))
    ramp = 1.0 + 2.0 * position
    factor = jax.random.uniform(gain_key, (D,), jnp.float32, 0.85, 1.15)
    return ramp * factor


def draw_w_keyval(key, part):
    return keyval_values(key).astype(jnp.bfloat16)


def draw_d_keyval(key, part):
    inputs = input_values(key)
    weights = keyval_values(key)
    scaled = inputs * lax.rsqrt(jnp.mean(inputs * inputs, axis=1, keepdims=True) + 1e-05)
    projected = jnp.dot(scaled, weights, precision=lax.Precision.HIGHEST)
    noise_key = jax.random.fold_in(key, 303)
    noise = jax.random.normal(noise_key, (TOKENS, KVW), jnp.float32)
    return jnp.clip(0.6 * projected + 0.8 * noise, -6.0, 6.0).astype(jnp.bfloat16)


def levels(own_key, shape, cuts, smallest, largest):
    def one(axis_at, blocks):
        heights = jax.random.uniform(jax.random.fold_in(jax.random.fold_in(own_key, 6), axis_at), (blocks,), jnp.float32, smallest / len(cuts), largest / len(cuts))
        return jnp.repeat(jnp.exp(heights), shape[axis_at] // blocks).reshape((-1,) + (1,) * (len(shape) - axis_at - 1))

    loudness = one(*cuts[0])
    for cut in cuts[1:]:
        loudness = loudness * one(*cut)
    return loudness


def bell_draw(rng, extent, deviation, bound, cuts=(), kind=jnp.bfloat16):
    entries = jax.random.normal(rng, extent, jnp.float32) * deviation
    if len(cuts) > 0:
        entries = levels(rng, extent, cuts, -0.22, 0.18) * entries
    return jnp.clip(entries, min=-bound, max=bound).astype(kind)


def setup_inputs(seed: int = 0) -> dict:
    arg_keys = jax.random.split(jax.random.key(seed), 8)
    layer_input = draw_layer_input(jax.random.fold_in(arg_keys[7], 71), 0)
    gain = draw_gain(jax.random.fold_in(arg_keys[7], 71), 0)
    d_query = bell_draw(arg_keys[2], (TOKENS, QW), 1.0, 6.0, ((0, 32), (1, 8)))
    d_keyval = draw_d_keyval(jax.random.fold_in(arg_keys[7], 71), 0)
    w_query = bell_draw(arg_keys[4], (D, QW), D ** -0.5, 0.0625, ((0, 32), (1, 8)))
    w_keyval = draw_w_keyval(jax.random.fold_in(arg_keys[7], 71), 0)
    d_resid = bell_draw(arg_keys[6], (TOKENS, D), 1.0, 6.0, ((0, 32), (1, 8)))
    return dict(layer_input=layer_input, gain=gain, d_query=d_query, d_keyval=d_keyval, w_query=w_query, w_keyval=w_keyval, d_resid=d_resid)


epsilon = 1e-05

def reference(layer_input, gain, d_query, d_keyval, w_query, w_keyval, d_resid):
    inputs = layer_input.astype(jnp.float32)
    inv_rms = lax.rsqrt(lax.optimization_barrier(jnp.mean(inputs * inputs, axis=1, keepdims=True)) + epsilon)
    normed = (inputs * inv_rms * gain).astype(jnp.bfloat16)
    query_cols = QW // N_COL
    keyval_cols = KVW // N_COL
    contract_cols = (((1,), (1,)), ((), ()))

    def add_block(block, accum_grad):
        qstart = (block * query_cols).astype(jnp.int32)
        kstart = (block * keyval_cols).astype(jnp.int32)
        qgrad = lax.dynamic_slice_in_dim(d_query, qstart, query_cols, 1)
        qweight = lax.dynamic_slice_in_dim(w_query, qstart, query_cols, 1)
        kgrad = lax.dynamic_slice_in_dim(d_keyval, kstart, keyval_cols, 1)
        kweight = lax.dynamic_slice_in_dim(w_keyval, kstart, keyval_cols, 1)
        partial_value = lax.dot_general(qgrad, qweight, contract_cols, preferred_element_type=jnp.float32)
        partial_value = partial_value + lax.dot_general(kgrad, kweight, contract_cols, preferred_element_type=jnp.float32)
        return accum_grad + partial_value.astype(jnp.bfloat16).astype(jnp.float32)
    feature_grad = lax.fori_loop(0, N_COL, add_block, jnp.zeros((TOKENS, D), jnp.float32))
    token_dot = lax.optimization_barrier(jnp.sum(gain * feature_grad * inputs, axis=1, keepdims=True))
    d_input = (d_resid.astype(jnp.float32) + inv_rms * gain * feature_grad - inputs * inv_rms ** 3 * token_dot / D).astype(jnp.bfloat16)
    scaling = 1.0 / jnp.sqrt(jnp.float32(TOKENS))
    grad_gain = lax.optimization_barrier(jnp.sum(feature_grad * inputs * inv_rms, axis=0)) * scaling
    weight_scale = 1.0 / jnp.sqrt(jnp.float32(TOK_DEV))
    contract_rows = (((0,), (0,)), ((), ()))

    def add_tokens(block, accums):
        tstart = (block * TOK_DEV).astype(jnp.int32)
        slab = lax.dynamic_slice_in_dim(normed, tstart, TOK_DEV, 0)
        qgrad = lax.dynamic_slice_in_dim(d_query, tstart, TOK_DEV, 0)
        kgrad = lax.dynamic_slice_in_dim(d_keyval, tstart, TOK_DEV, 0)
        block_q = lax.dot_general(slab, qgrad, contract_rows, preferred_element_type=jnp.float32) * weight_scale
        block_kv = lax.dot_general(slab, kgrad, contract_rows, preferred_element_type=jnp.float32) * weight_scale
        return (accums[0] + block_q.astype(jnp.bfloat16).astype(jnp.float32), accums[1] + block_kv.astype(jnp.bfloat16).astype(jnp.float32))
    sum_q, sum_kv = lax.fori_loop(0, N_ROW, add_tokens, (jnp.zeros((D, QW), jnp.float32), jnp.zeros((D, KVW), jnp.float32)))
    grad_wq = sum_q.astype(jnp.bfloat16)
    grad_wkv = sum_kv.astype(jnp.bfloat16)
    query_f = grad_wq.astype(jnp.float32)
    keyval_f = grad_wkv.astype(jnp.float32)
    grand_total = jnp.sum(query_f * query_f) + jnp.sum(keyval_f * keyval_f) + jnp.sum(grad_gain * grad_gain)
    grad_square_sum = grand_total / jnp.float32(D)
    return (d_input, grad_wq, grad_wkv, grad_gain, grad_square_sum)
```

```python
import math

import jax
import jax.numpy as jnp
from jax import lax
from jax.sharding import Mesh
from jax.sharding import PartitionSpec as P

ROW = ("y", "z")
COL = ("x", "k")
f32 = jnp.float32
bf16 = jnp.bfloat16

epsilon = 1e-05


def copies(block, axis):
    count = lax.axis_size(axis)
    spread = jnp.broadcast_to(block[None], (count, *block.shape))
    return lax.all_to_all(spread, axis, 0, 0, tiled=True)


def local(layer_input, gain, d_query, d_keyval, w_query, w_keyval, d_resid):
    ny, nz, nx, nk = (lax.axis_size(a) for a in ("y", "z", "x", "k"))
    y, z, x, k = (lax.axis_index(a) for a in ("y", "z", "x", "k"))
    tokens, width = layer_input.shape
    all_tokens = tokens * ny * nz
    part = width // ny
    half = part // nk
    rows = part // nz
    query_cols = d_query.shape[1]
    col = x * nk + k

    w_tile = jnp.concatenate([w_query, w_keyval], axis=1)
    w_part = lax.all_gather(w_tile, "z", axis=0, tiled=True)
    d_tile = jnp.concatenate([d_query, d_keyval], axis=1)
    d_part = copies(d_tile, "y")
    columns = d_tile.shape[1]

    share = tokens // (nx * nk)
    mine = lax.dynamic_slice_in_dim(layer_input, col * share, share, 0).astype(f32)
    scale = lax.rsqrt(jnp.mean(mine * mine, axis=1, keepdims=True) + epsilon)
    normed = (mine * scale * gain).astype(bf16)
    normed = jnp.moveaxis(normed.reshape(share, ny, part), 1, 0)
    normed = lax.all_to_all(normed, "y", 0, 0, tiled=True)
    normed = lax.all_gather(normed[None], COL, axis=0, tiled=True)

    d_rows = d_part.reshape(ny * tokens, columns)
    contract_cols = (((1,), (1,)), ((), ()))
    w_other = lax.dynamic_slice_in_dim(w_part, (1 - k) * half, half, 0)
    w_own = lax.dynamic_slice_in_dim(w_part, k * half, half, 0)
    other = lax.dot_general(d_rows, w_other, contract_cols, preferred_element_type=f32)
    other = lax.ppermute(other.astype(bf16), "k", [(0, 1), (1, 0)])
    own = lax.dot_general(d_rows, w_own, contract_cols, preferred_element_type=f32)
    both = (own + other.astype(f32)).astype(bf16).reshape(ny, tokens, half)
    pieces = lax.all_to_all(both, "x", 0, 0, tiled=True)
    summed = jnp.sum(pieces.astype(f32), axis=0).astype(bf16)
    swap = [(a * nx + b, b * nx + a) for a in range(ny) for b in range(nx)]
    feature_grad = lax.ppermute(summed, ("y", "x"), swap).astype(f32)

    inputs = layer_input.astype(f32)
    inv_rms = lax.rsqrt(jnp.mean(inputs * inputs, axis=1, keepdims=True) + epsilon)
    input_part = lax.dynamic_slice_in_dim(layer_input, col * half, half, 1).astype(f32)
    gain_part = lax.dynamic_slice_in_dim(gain, col * half, half, 0)
    weighted = gain_part * feature_grad
    dots = jnp.sum(weighted * input_part, axis=1)
    token_dot = jnp.sum(copies(dots, COL), axis=0)[:, None]
    d_input = (
        d_resid.astype(f32)
        + inv_rms * weighted
        - input_part * inv_rms**3 * token_dot / width
    ).astype(bf16)

    d_sorted = jnp.moveaxis(d_part.reshape(ny, nx * nk, share, columns), 1, 0)
    weight_scale = 1.0 / math.sqrt(tokens)
    tile_partial = lax.dot_general(
        normed.reshape(nx * nk * ny * share, part),
        d_sorted.reshape(nx * nk * ny * share, columns),
        (((0,), (0,)), ((), ())),
        preferred_element_type=f32,
    )
    tile_partial = (tile_partial * weight_scale).astype(bf16)
    tile = lax.psum_scatter(tile_partial, "z", scatter_dimension=0, tiled=True)
    grad_wq = tile[:, :query_cols]
    grad_wkv = tile[:, query_cols:]
    tile_f = tile.astype(f32)
    tile_square = jnp.sum(tile_f * tile_f)

    row = y * nz + z
    gain_row = lax.dynamic_slice_in_dim(gain, row * rows, rows, 0)
    gain_scale = 1.0 / (weight_scale * math.sqrt(all_tokens))
    gain_terms = jnp.sum(tile_f * w_tile.astype(f32), axis=1) * gain_scale / gain_row
    packed = jnp.concatenate([gain_terms, jnp.broadcast_to(tile_square, (128,))])
    packed = jnp.sum(copies(packed.reshape(-1, 128), COL), axis=0)
    packed = copies(packed, ROW)
    packed = packed.reshape(ny * nz, rows + 128)
    gains = packed[:, :rows].reshape(width)
    grand_total = jnp.sum(packed[:, rows]) + jnp.sum(gains * gains)
    grad_square_sum = grand_total / f32(width)
    grad_gain = lax.dynamic_slice_in_dim(gains, col * half, half, 0)
    return (d_input, grad_wq, grad_wkv, grad_gain, grad_square_sum)


def solution(mesh):
    torus = Mesh(mesh.devices.reshape(4, 8, 4, 2), ("y", "z", "x", "k"))
    both = P(ROW, COL)
    in_specs = (P(ROW, None), P(), both, both, both, both, both)
    out_specs = (both, both, both, P(COL), P())
    return jax.shard_map(local, mesh=torus, in_specs=in_specs, out_specs=out_specs, check_vma=False)
```

```python
import math

import jax
import jax.numpy as jnp
from jax import lax
from jax.sharding import Mesh
from jax.sharding import PartitionSpec as P


ROW = ("y", "z")
COL = ("x", "k")
CHUNKS = 2
f32 = jnp.float32
bf16 = jnp.bfloat16

epsilon = 1e-05


def shifted(block, axis, step):
    count = lax.axis_size(axis)
    if step % count == 0:
        return block
    ring = [(i, (i + step) % count) for i in range(count)]
    return lax.ppermute(block, axis, ring)


def added(block, axis):
    count = lax.axis_size(axis)
    return sum(shifted(block, axis, s) for s in range(1, count)) + block


def copies(block, axis):
    count = lax.axis_size(axis)
    spread = jnp.broadcast_to(block[None], (count, *block.shape))
    return lax.all_to_all(spread, axis, 0, 0, tiled=True)


def cut(array, at, size, axis):
    return lax.dynamic_slice_in_dim(array, at, size, axis)


def local(layer_input, gain, d_query, d_keyval, w_query, w_keyval, d_resid):
    ny, nz, nx, nk = (lax.axis_size(a) for a in ("y", "z", "x", "k"))
    y, z, x, k = (lax.axis_index(a) for a in ("y", "z", "x", "k"))
    tokens, width = layer_input.shape
    all_tokens = tokens * ny * nz
    part = width // ny
    half = part // nk
    rows = part // nz
    query_cols = d_query.shape[1]
    col = x * nk + k

    w_tile = jnp.concatenate([w_query, w_keyval], axis=1)
    w_part = lax.all_gather(w_tile, "z", axis=0, tiled=True)

    share = tokens // (nx * nk)
    mine = cut(layer_input, col * share, share, 0).astype(f32)
    scale = lax.rsqrt(jnp.mean(mine * mine, axis=1, keepdims=True) + epsilon)
    normed = (mine * scale * gain).astype(bf16)
    over_y = [
        shifted(cut(normed, lax.rem(y + s, ny) * part, part, 1), "y", s)
        for s in range(ny)
    ]
    over_y = jnp.stack(over_y)

    d_tile = jnp.concatenate([d_query, d_keyval], axis=1)
    columns = d_tile.shape[1]
    d_part = jnp.stack([shifted(d_tile, "y", s) for s in range(ny)])

    over_x = jnp.stack([shifted(over_y, "x", -s) for s in range(nx)])
    over_x, d_part = lax.optimization_barrier((over_x, d_part))
    over_k = jnp.stack([over_x, shifted(over_x, "k", 1)])

    weight_scale = 1.0 / math.sqrt(tokens)
    d_sorted = d_part.reshape(ny, nx, nk, share, columns)
    d_sorted = jnp.where(k == 0, d_sorted, jnp.flip(d_sorted, 2))
    d_sorted = cut(jnp.concatenate([d_sorted, d_sorted], axis=1), x, nx, 1)
    d_sorted = d_sorted.transpose(2, 1, 0, 3, 4)
    tile_partial = lax.dot_general(
        over_k.reshape(ny * tokens, part),
        d_sorted.reshape(ny * tokens, columns),
        (((0,), (0,)), ((), ())),
        preferred_element_type=f32,
    )
    tile_partial = (tile_partial * weight_scale).astype(bf16)
    tile = lax.psum_scatter(tile_partial, "z", scatter_dimension=0, tiled=True)
    grad_wq = tile[:, :query_cols]
    grad_wkv = tile[:, query_cols:]
    tile_f = tile.astype(f32)
    tile_square = jnp.sum(tile_f * tile_f)

    contract_cols = (((1,), (1,)), ((), ()))
    w_other = cut(w_part, (1 - k) * half, half, 0)
    w_own = cut(w_part, k * half, half, 0)
    step = tokens // CHUNKS
    placed = []
    for c in range(CHUNKS):
        d_rows = d_part[:, c * step : (c + 1) * step].reshape(ny * step, columns)
        other = lax.dot_general(d_rows, w_other, contract_cols, preferred_element_type=f32)
        other = shifted(other.astype(bf16), "k", 1)
        own = lax.dot_general(d_rows, w_own, contract_cols, preferred_element_type=f32)
        both = (own + other.astype(f32)).astype(bf16).reshape(ny, step, half)
        home = jnp.stack([shifted(both[s], "y", -s) for s in range(ny)])
        arrived = [
            shifted(lax.dynamic_index_in_dim(home, lax.rem(x + s - y + ny, ny), 0, False), "x", s)
            for s in range(nx)
        ]
        placed.append(sum(a.astype(f32) for a in arrived))
    feature_grad = jnp.concatenate(placed, axis=0)

    inputs = layer_input.astype(f32)
    inv_rms = lax.rsqrt(jnp.mean(inputs * inputs, axis=1, keepdims=True) + epsilon)
    input_part = cut(layer_input, col * half, half, 1).astype(f32)
    gain_part = cut(gain, col * half, half, 0)
    weighted = gain_part * feature_grad
    dots = jnp.sum(weighted * input_part, axis=1)
    token_dot = added(added(dots, "k"), "x")[:, None]
    d_input = (
        d_resid.astype(f32)
        + inv_rms * weighted
        - input_part * inv_rms**3 * token_dot / width
    ).astype(bf16)

    row = y * nz + z
    gain_row = cut(gain, row * rows, rows, 0)
    gain_scale = 1.0 / (weight_scale * math.sqrt(all_tokens))
    gain_terms = jnp.sum(tile_f * w_tile.astype(f32), axis=1) * gain_scale / gain_row
    packed = jnp.concatenate([gain_terms, jnp.broadcast_to(tile_square, (128,))])
    packed = added(added(packed.reshape(-1, 128), "k"), "x")
    packed = copies(packed, ROW)
    packed = packed.reshape(ny * nz, rows + 128)
    gains = packed[:, :rows].reshape(width)
    grand_total = jnp.sum(packed[:, rows]) + jnp.sum(gains * gains)
    grad_square_sum = grand_total / f32(width)
    grad_gain = cut(gains, col * half, half, 0)
    return (d_input, grad_wq, grad_wkv, grad_gain, grad_square_sum)


def solution(mesh):
    torus = Mesh(mesh.devices.reshape(4, 8, 4, 2), ("y", "z", "x", "k"))
    both = P(ROW, COL)
    in_specs = (P(ROW, None), P(), both, both, both, both, both)
    out_specs = (both, both, both, P(COL), P())
    return jax.shard_map(local, mesh=torus, in_specs=in_specs, out_specs=out_specs, check_vma=False)
```

```python
import math

import jax
import jax.numpy as jnp
from jax import lax
from jax.sharding import Mesh
from jax.sharding import PartitionSpec as P


ROW = ("y", "z")
COL = ("x", "k")
CHUNKS = 2
f32 = jnp.float32
bf16 = jnp.bfloat16

epsilon = 1e-05


def shifted(block, axis, step):
    count = lax.axis_size(axis)
    if step % count == 0:
        return block
    ring = [(i, (i + step) % count) for i in range(count)]
    return lax.ppermute(block, axis, ring)


def copies(block, axis):
    count = lax.axis_size(axis)
    spread = jnp.broadcast_to(block[None], (count, *block.shape))
    return lax.all_to_all(spread, axis, 0, 0, tiled=True)


def cut(array, at, size, axis):
    return lax.dynamic_slice_in_dim(array, at, size, axis)


def local(layer_input, gain, d_query, d_keyval, w_query, w_keyval, d_resid):
    ny, nz, nx, nk = (lax.axis_size(a) for a in ("y", "z", "x", "k"))
    y, z, x, k = (lax.axis_index(a) for a in ("y", "z", "x", "k"))
    tokens, width = layer_input.shape
    all_tokens = tokens * ny * nz
    part = width // ny
    half = part // nk
    rows = part // nz
    query_cols = d_query.shape[1]
    col = x * nk + k

    w_tile = jnp.concatenate([w_query, w_keyval], axis=1)
    w_tile, layer_input = lax.optimization_barrier((w_tile, layer_input))
    w_part = lax.all_gather(w_tile, "z", axis=0, tiled=True)

    share = tokens // (nx * nk)
    mine = cut(layer_input, col * share, share, 0).astype(f32)
    scale = lax.rsqrt(jnp.mean(mine * mine, axis=1, keepdims=True) + epsilon)
    normed = (mine * scale * gain).astype(bf16)
    over_y = [
        shifted(cut(normed, lax.rem(y + s, ny) * part, part, 1), "y", s)
        for s in range(1, ny)
    ]
    over_y = jnp.stack(over_y)

    d_tile = jnp.concatenate([d_query, d_keyval], axis=1)
    columns = d_tile.shape[1]
    d_part = jnp.stack([shifted(d_tile, "y", s) for s in range(ny)])

    over_x = jnp.stack([shifted(over_y, "x", -s) for s in range(nx)], axis=1)
    over_x, d_part = lax.optimization_barrier((over_x, d_part))
    over_k = shifted(over_x, "k", 1)

    inputs = layer_input.astype(f32)
    inv_rms = lax.rsqrt(jnp.mean(inputs * inputs, axis=1, keepdims=True) + epsilon)
    own_input = cut(layer_input, y * part, part, 1).astype(f32)
    own_normed = (own_input * inv_rms * cut(gain, y * part, part, 0)).astype(bf16)

    weight_scale = 1.0 / math.sqrt(tokens)
    contract_rows = (((0,), (0,)), ((), ()))
    tile_partial = lax.dot_general(
        own_normed, d_tile, contract_rows, preferred_element_type=f32
    )
    d_shares = d_part[1:].reshape(ny - 1, nx, nk, share, columns)
    for core, theirs in ((k, over_x), (1 - k, over_k)):
        d_core = cut(d_shares, core, 1, 2)[:, :, 0]
        d_core = cut(jnp.concatenate([d_core, d_core], axis=1), x, nx, 1)
        tile_partial = tile_partial + lax.dot_general(
            theirs.reshape(-1, part),
            d_core.reshape(-1, columns),
            contract_rows,
            preferred_element_type=f32,
        )
    tile_partial = (tile_partial * weight_scale).astype(bf16)
    tile = lax.psum_scatter(tile_partial, "z", scatter_dimension=0, tiled=True)
    grad_wq = tile[:, :query_cols]
    grad_wkv = tile[:, query_cols:]
    tile_f = tile.astype(f32)
    tile_square = jnp.sum(tile_f * tile_f)

    row = y * nz + z
    gain_row = cut(gain, row * rows, rows, 0)
    gain_scale = 1.0 / (weight_scale * math.sqrt(all_tokens))
    gain_terms = jnp.sum(tile_f * w_tile.astype(f32), axis=1) * gain_scale / gain_row
    packed = jnp.concatenate([gain_terms, jnp.broadcast_to(tile_square, (128,))])
    packed = jnp.sum(copies(packed.reshape(-1, 128), COL), axis=0)

    contract_cols = (((1,), (1,)), ((), ()))
    w_other = cut(w_part, (1 - k) * half, half, 0)
    w_own = cut(w_part, k * half, half, 0)
    step = tokens // CHUNKS
    placed = []
    for c in range(CHUNKS):
        d_rows = d_part[:, c * step : (c + 1) * step].reshape(ny * step, columns)
        other = lax.dot_general(d_rows, w_other, contract_cols, preferred_element_type=f32)
        other = shifted(other.astype(bf16), "k", 1)
        own = lax.dot_general(d_rows, w_own, contract_cols, preferred_element_type=f32)
        both = (own + other.astype(f32)).astype(bf16).reshape(ny, step, half)
        home = jnp.stack([shifted(both[s], "y", -s) for s in range(ny)])
        arrived = [
            shifted(lax.dynamic_index_in_dim(home, lax.rem(x + s - y + ny, ny), 0, False), "x", s)
            for s in range(nx)
        ]
        placed.append(arrived)
    placed[-1], packed = lax.optimization_barrier((placed[-1], packed))
    feature_grad = jnp.concatenate(
        [sum(a.astype(f32) for a in arrived) for arrived in placed], axis=0
    )

    input_part = cut(layer_input, col * half, half, 1).astype(f32)
    gain_part = cut(gain, col * half, half, 0)
    weighted = gain_part * feature_grad
    dots = jnp.sum(weighted * input_part, axis=1)
    token_dot = jnp.sum(copies(dots, COL), axis=0)[:, None]
    d_input = (
        d_resid.astype(f32)
        + inv_rms * weighted
        - input_part * inv_rms**3 * token_dot / width
    ).astype(bf16)

    packed = copies(packed, ROW)
    packed = packed.reshape(ny * nz, rows + 128)
    gains = packed[:, :rows].reshape(width)
    grand_total = jnp.sum(packed[:, rows]) + jnp.sum(gains * gains)
    grad_square_sum = grand_total / f32(width)
    grad_gain = cut(gains, col * half, half, 0)
    return (d_input, grad_wq, grad_wkv, grad_gain, grad_square_sum)


def solution(mesh):
    torus = Mesh(mesh.devices.reshape(4, 8, 4, 2), ("y", "z", "x", "k"))
    both = P(ROW, COL)
    in_specs = (P(ROW, None), P(), both, both, both, both, both)
    out_specs = (both, both, both, P(COL), P())
    return jax.shard_map(local, mesh=torus, in_specs=in_specs, out_specs=out_specs, check_vma=False)
```

```python
import math

import jax
import jax.numpy as jnp
from jax import lax
from jax.sharding import Mesh
from jax.sharding import PartitionSpec as P


ROW = ("y", "z")
COL = ("x", "k")
CHUNKS = 2
f32 = jnp.float32
bf16 = jnp.bfloat16

epsilon = 1e-05


def shifted(block, axis, step):
    count = lax.axis_size(axis)
    if step % count == 0:
        return block
    ring = [(i, (i + step) % count) for i in range(count)]
    return lax.ppermute(block, axis, ring)


def copies(block, axis):
    count = lax.axis_size(axis)
    spread = jnp.broadcast_to(block[None], (count, *block.shape))
    return lax.all_to_all(spread, axis, 0, 0, tiled=True)


def cut(array, at, size, axis):
    return lax.dynamic_slice_in_dim(array, at, size, axis)


def local(layer_input, gain, d_query, d_keyval, w_query, w_keyval, d_resid):
    ny, nz, nx, nk = (lax.axis_size(a) for a in ("y", "z", "x", "k"))
    y, z, x, k = (lax.axis_index(a) for a in ("y", "z", "x", "k"))
    tokens, width = layer_input.shape
    all_tokens = tokens * ny * nz
    part = width // ny
    half = part // nk
    rows = part // nz
    query_cols = d_query.shape[1]
    col = x * nk + k

    w_tile = jnp.concatenate([w_query, w_keyval], axis=1)
    w_tile, layer_input = lax.optimization_barrier((w_tile, layer_input))
    w_part = lax.all_gather(w_tile, "z", axis=0, tiled=True)

    share = tokens // (nx * nk)
    mine = cut(layer_input, col * share, share, 0).astype(f32)
    scale = lax.rsqrt(jnp.mean(mine * mine, axis=1, keepdims=True) + epsilon)
    normed = (mine * scale * gain).astype(bf16)
    over_y = [
        shifted(cut(normed, lax.rem(y + s, ny) * part, part, 1), "y", s)
        for s in range(1, ny)
    ]
    over_y = jnp.stack(over_y)

    d_tile = jnp.concatenate([d_query, d_keyval], axis=1)
    columns = d_tile.shape[1]
    d_part = jnp.stack([shifted(d_tile, "y", s) for s in range(ny)])

    over_x = jnp.stack([shifted(over_y, "x", -s) for s in range(nx)], axis=1)
    over_x, d_part = lax.optimization_barrier((over_x, d_part))
    over_k = shifted(over_x, "k", 1)

    inputs = layer_input.astype(f32)
    inv_rms = lax.rsqrt(jnp.mean(inputs * inputs, axis=1, keepdims=True) + epsilon)
    own_input = cut(layer_input, y * part, part, 1).astype(f32)
    own_normed = (own_input * inv_rms * cut(gain, y * part, part, 0)).astype(bf16)

    weight_scale = 1.0 / math.sqrt(tokens)
    contract_rows = (((0,), (0,)), ((), ()))
    tile_partial = lax.dot_general(
        own_normed, d_tile, contract_rows, preferred_element_type=f32
    )
    d_shares = d_part[1:].reshape(ny - 1, nx, nk, share, columns)
    for core, theirs in ((k, over_x), (1 - k, over_k)):
        d_core = cut(d_shares, core, 1, 2)[:, :, 0]
        d_core = cut(jnp.concatenate([d_core, d_core], axis=1), x, nx, 1)
        tile_partial = tile_partial + lax.dot_general(
            theirs.reshape(-1, part),
            d_core.reshape(-1, columns),
            contract_rows,
            preferred_element_type=f32,
        )
    tile_partial = (tile_partial * weight_scale).astype(bf16)
    tile = lax.psum_scatter(tile_partial, "z", scatter_dimension=0, tiled=True)
    grad_wq = tile[:, :query_cols]
    grad_wkv = tile[:, query_cols:]
    tile_f = tile.astype(f32)
    tile_square = jnp.sum(tile_f * tile_f)

    contract_cols = (((1,), (1,)), ((), ()))
    w_other = cut(w_part, (1 - k) * half, half, 0)
    w_own = cut(w_part, k * half, half, 0)
    step = tokens // CHUNKS
    placed, homes = [], []
    for c in range(CHUNKS):
        d_rows = d_part[:, c * step : (c + 1) * step].reshape(ny * step, columns)
        other = lax.dot_general(d_rows, w_other, contract_cols, preferred_element_type=f32)
        other = shifted(other.astype(bf16), "k", 1)
        own = lax.dot_general(d_rows, w_own, contract_cols, preferred_element_type=f32)
        both = (own + other.astype(f32)).astype(bf16).reshape(ny, step, half)
        home = jnp.stack([shifted(both[s], "y", -s) for s in range(ny)])
        homes.append(home)
        arrived = [
            shifted(lax.dynamic_index_in_dim(home, lax.rem(x + s - y + ny, ny), 0, False), "x", s)
            for s in range(nx)
        ]
        placed.append(arrived)
    dots = 0.0
    for s in range(ny):
        at = lax.rem(y + s, ny) * part + k * half
        piece = jnp.concatenate([home[s] for home in homes], axis=0).astype(f32)
        their_input = cut(layer_input, at, half, 1).astype(f32)
        dots = dots + jnp.sum(piece * their_input * cut(gain, at, half, 0), axis=1)

    row = y * nz + z
    gain_row = cut(gain, row * rows, rows, 0)
    gain_scale = 1.0 / (weight_scale * math.sqrt(all_tokens))
    gain_terms = jnp.sum(tile_f * w_tile.astype(f32), axis=1) * gain_scale / gain_row

    lanes = 128
    packed = jnp.concatenate([gain_terms, jnp.broadcast_to(tile_square / lanes, (lanes,)), dots])
    packed = jnp.sum(copies(packed.reshape(-1, lanes), COL), axis=0)
    placed[-1], _ = lax.optimization_barrier((placed[-1], packed))
    split = rows // lanes + 1
    token_dot = packed[split:].reshape(tokens, 1)
    packed = copies(packed[:split], ROW)
    feature_grad = jnp.concatenate(
        [sum(a.astype(f32) for a in arrived) for arrived in placed], axis=0
    )

    input_part = cut(layer_input, col * half, half, 1).astype(f32)
    gain_part = cut(gain, col * half, half, 0)
    weighted = gain_part * feature_grad
    d_input = (
        d_resid.astype(f32)
        + inv_rms * weighted
        - input_part * inv_rms**3 * token_dot / width
    ).astype(bf16)

    is_square = lax.broadcasted_iota(jnp.int32, packed.shape, 1) == split - 1
    grand_total = jnp.sum(jnp.where(is_square, packed, packed * packed))
    grad_square_sum = grand_total / f32(width)
    per_col = ny * nz // (nx * nk)
    grad_gain = cut(packed, col * per_col, per_col, 0)[:, : split - 1].reshape(half)
    return (d_input, grad_wq, grad_wkv, grad_gain, grad_square_sum)


def solution(mesh):
    torus = Mesh(mesh.devices.reshape(4, 8, 4, 2), ("y", "z", "x", "k"))
    both = P(ROW, COL)
    in_specs = (P(ROW, None), P(), both, both, both, both, both)
    out_specs = (both, both, both, P(COL), P())
    return jax.shard_map(local, mesh=torus, in_specs=in_specs, out_specs=out_specs, check_vma=False)
```

```python
import math

import jax
import jax.numpy as jnp
from jax import lax
from jax.sharding import Mesh
from jax.sharding import PartitionSpec as P


ROW = ("y", "z")
COL = ("x", "k")
f32 = jnp.float32
bf16 = jnp.bfloat16

epsilon = 1e-05


def shifted(block, axis, step):
    count = lax.axis_size(axis)
    if step % count == 0:
        return block
    ring = [(i, (i + step) % count) for i in range(count)]
    return lax.ppermute(block, axis, ring)


def copies(block, axis):
    count = lax.axis_size(axis)
    spread = jnp.broadcast_to(block[None], (count, *block.shape))
    return lax.all_to_all(spread, axis, 0, 0, tiled=True)


def cut(array, at, size, axis):
    return lax.dynamic_slice_in_dim(array, at, size, axis)


def local(layer_input, gain, d_query, d_keyval, w_query, w_keyval, d_resid):
    ny, nz, nx, nk = (lax.axis_size(a) for a in ("y", "z", "x", "k"))
    y, z, x, k = (lax.axis_index(a) for a in ("y", "z", "x", "k"))
    tokens, width = layer_input.shape
    all_tokens = tokens * ny * nz
    part = width // ny
    half = part // nk
    rows = part // nz
    query_cols = d_query.shape[1]
    col = x * nk + k

    d_tile = jnp.concatenate([d_query, d_keyval], axis=1)
    d_tile, layer_input = lax.optimization_barrier((d_tile, layer_input))
    columns = d_tile.shape[1]
    d_all = lax.all_gather(d_tile, ("k", "z"), axis=0, tiled=True)
    d_all = d_all.reshape(nk, nz, tokens, columns)

    share = tokens // (nx * nk)
    mine = cut(layer_input, col * share, share, 0).astype(f32)
    scale = lax.rsqrt(jnp.mean(mine * mine, axis=1, keepdims=True) + epsilon)
    normed = (mine * scale * gain).astype(bf16)
    normed = jnp.stack(
        [
            cut(normed, lax.rem(y + r, ny) * part, part, 1).reshape(share, nz, rows)
            for r in range(ny)
        ],
        axis=2,
    )
    normed = jnp.moveaxis(normed, 1, 0).reshape(nz, share, ny * rows)
    over_z = lax.all_to_all(normed, "z", 0, 0, tiled=True)

    w_tile = jnp.concatenate([w_query, w_keyval], axis=1)
    w_part = jnp.stack([shifted(w_tile, "y", s) for s in range(ny)])

    over_x = jnp.stack([shifted(over_z, "x", -s) for s in range(nx)], axis=1)
    over_x, w_part = lax.optimization_barrier((over_x, w_part))
    over_k = shifted(over_x, "k", 1)
    w_other = shifted(w_part, "k", 1)

    contract_cols = (((1,), (1,)), ((), ()))
    few = tokens // nk
    d_half = cut(d_all, k * few, few, 2)
    grad_part = 0.0
    for core, weights in ((k, w_part), (1 - k, w_other)):
        grad_part = grad_part + lax.dot_general(
            lax.dynamic_index_in_dim(d_half, core, 0, False).reshape(nz * few, columns),
            weights.reshape(ny * rows, columns),
            contract_cols,
            preferred_element_type=f32,
        )
    grad_part = grad_part.astype(bf16)
    arrived = [
        shifted(cut(grad_part, lax.rem(y - x - u + 2 * ny, ny) * rows, rows, 1), "x", u)
        for u in range(nx)
    ]

    weight_scale = 1.0 / math.sqrt(tokens)
    contract_rows = (((0,), (0,)), ((), ()))
    d_shares = lax.dynamic_index_in_dim(d_all, k, 0, False)
    d_shares = d_shares.reshape(nz, nx, nk, share, columns)
    tile_partial = 0.0
    for core, theirs in ((k, over_x), (1 - k, over_k)):
        d_core = cut(d_shares, core, 1, 2)[:, :, 0]
        d_core = cut(jnp.concatenate([d_core, d_core], axis=1), x, nx, 1)
        tile_partial = tile_partial + lax.dot_general(
            theirs.reshape(-1, ny * rows),
            d_core.reshape(-1, columns),
            contract_rows,
            preferred_element_type=f32,
        )
    tile_partial = (tile_partial * weight_scale).astype(bf16).reshape(ny, rows, columns)
    tile = sum(shifted(tile_partial[r], "y", r).astype(f32) for r in range(ny)).astype(bf16)
    grad_wq = tile[:, :query_cols]
    grad_wkv = tile[:, query_cols:]
    tile_f = tile.astype(f32)
    tile_square = jnp.sum(tile_f * tile_f)

    row = y * nz + z
    gain_row = cut(gain, row * rows, rows, 0)
    gain_scale = 1.0 / (weight_scale * math.sqrt(all_tokens))
    gain_terms = jnp.sum(tile_f * w_tile.astype(f32), axis=1) * gain_scale / gain_row
    lanes = 128
    packed = jnp.concatenate([gain_terms, jnp.broadcast_to(tile_square / lanes, (lanes,))])
    packed = jnp.sum(copies(packed.reshape(-1, lanes), COL), axis=0)
    split = rows // lanes
    packed = copies(packed, ROW)

    placed = sum(a.astype(f32) for a in arrived).astype(bf16).reshape(nz, few, rows)
    placed = lax.all_to_all(placed, "z", 0, 0, tiled=True)
    placed = jnp.moveaxis(placed, 0, 1).reshape(few, part)
    their_input = cut(cut(layer_input, k * few, few, 0), x * part, part, 1).astype(f32)
    dots = jnp.sum(placed.astype(f32) * their_input * cut(gain, x * part, part, 0), axis=1)
    dots = sum(shifted(dots, "x", u) for u in range(nx))

    def by_half(own, other):
        return jnp.concatenate(
            [jnp.where(k == 0, own, other), jnp.where(k == 0, other, own)], axis=0
        )

    token_dot = by_half(dots, shifted(dots, "k", 1))[:, None]
    own_grad = cut(placed, k * half, half, 1)
    other_grad = shifted(cut(placed, (1 - k) * half, half, 1), "k", 1)
    feature_grad = by_half(own_grad, other_grad).astype(f32)

    inputs = layer_input.astype(f32)
    inv_rms = lax.rsqrt(jnp.mean(inputs * inputs, axis=1, keepdims=True) + epsilon)
    input_part = cut(layer_input, col * half, half, 1).astype(f32)
    weighted = cut(gain, col * half, half, 0) * feature_grad
    d_input = (
        d_resid.astype(f32)
        + inv_rms * weighted
        - input_part * inv_rms**3 * token_dot / width
    ).astype(bf16)

    is_square = lax.broadcasted_iota(jnp.int32, packed.shape, 1) == split
    grand_total = jnp.sum(jnp.where(is_square, packed, packed * packed))
    grad_square_sum = grand_total / f32(width)
    per_col = ny * nz // (nx * nk)
    grad_gain = cut(packed, col * per_col, per_col, 0)[:, :split].reshape(half)
    return (d_input, grad_wq, grad_wkv, grad_gain, grad_square_sum)


def solution(mesh):
    torus = Mesh(mesh.devices.reshape(4, 8, 4, 2), ("y", "z", "x", "k"))
    both = P(ROW, COL)
    in_specs = (P(ROW, None), P(), both, both, both, both, both)
    out_specs = (both, both, both, P(COL), P())
    return jax.shard_map(local, mesh=torus, in_specs=in_specs, out_specs=out_specs, check_vma=False)
```

```python
import math

import jax
import jax.numpy as jnp
from jax import lax
from jax.sharding import Mesh
from jax.sharding import PartitionSpec as P


ROW = ("y", "z")
COL = ("x", "k")
f32 = jnp.float32
bf16 = jnp.bfloat16

epsilon = 1e-05


def shifted(block, axis, step):
    count = lax.axis_size(axis)
    if step % count == 0:
        return block
    ring = [(i, (i + step) % count) for i in range(count)]
    return lax.ppermute(block, axis, ring)


def added(block, axis):
    count = lax.axis_size(axis)
    return sum(shifted(block, axis, s) for s in range(1, count)) + block


def copies(block, axis):
    count = lax.axis_size(axis)
    spread = jnp.broadcast_to(block[None], (count, *block.shape))
    return lax.all_to_all(spread, axis, 0, 0, tiled=True)


def rolled(blocks, first):
    count = blocks.shape[0]
    twice = jnp.concatenate([blocks, blocks], axis=0)
    return cut(twice, lax.rem(count - first, count), count, 0)


def cut(array, at, size, axis):
    return lax.dynamic_slice_in_dim(array, at, size, axis)


def local(layer_input, gain, d_query, d_keyval, w_query, w_keyval, d_resid):
    ny, nz, nx, nk = (lax.axis_size(a) for a in ("y", "z", "x", "k"))
    y, z, x, k = (lax.axis_index(a) for a in ("y", "z", "x", "k"))
    tokens, width = layer_input.shape
    all_tokens = tokens * ny * nz
    part = width // ny
    half = part // nk
    rows = part // nz
    query_cols = d_query.shape[1]
    col = x * nk + k

    d_tile = jnp.concatenate([d_query, d_keyval], axis=1)
    d_tile, layer_input = lax.optimization_barrier((d_tile, layer_input))
    columns = d_tile.shape[1]
    few = tokens // nk
    after, before = [d_tile], [d_tile]
    for _ in range(nz // 2 - 1):
        after.append(shifted(after[-1], "z", -1))
        before.append(shifted(before[-1], "z", 1))
    far = jnp.concatenate(
        [shifted(before[-1][:few], "z", 1), shifted(after[-1][few:], "z", -1)], axis=0
    )
    d_all = jnp.stack(after + [far] + before[:0:-1])
    near = len(after) - 1
    early = after[:near] + before[near - 1 : 0 : -1]
    late = [after[near], far, before[near]]
    early, late = (
        shifted(jnp.stack([cut(b, (1 - k) * few, few, 0) for b in blocks]), "k", 1)
        for blocks in (early, late)
    )
    d_other = jnp.concatenate([early[:near], late, early[near:]], axis=0)

    share = tokens // (nx * nk)
    mine = cut(layer_input, col * share, share, 0).astype(f32)
    scale = lax.rsqrt(jnp.mean(mine * mine, axis=1, keepdims=True) + epsilon)
    normed = (mine * scale * gain).astype(bf16)
    normed = jnp.stack(
        [
            cut(normed, lax.rem(y + r, ny) * part, part, 1).reshape(share, nz, rows)
            for r in range(ny)
        ],
        axis=2,
    )
    normed = jnp.moveaxis(normed, 1, 0).reshape(nz, share, ny * rows)
    over_z = lax.all_to_all(normed, "z", 0, 0, tiled=True)
    over_z = cut(jnp.concatenate([over_z, over_z], axis=0), z, nz, 0)

    w_tile = jnp.concatenate([w_query, w_keyval], axis=1)
    w_part = jnp.stack([shifted(w_tile, "y", s) for s in range(ny)])

    over_x = jnp.stack([shifted(over_z, "x", -s) for s in range(nx)], axis=1)
    over_x, w_part = lax.optimization_barrier((over_x, w_part))
    over_k = shifted(over_x, "k", 1)
    w_other = shifted(w_part, "k", 1)

    contract_cols = (((1,), (1,)), ((), ()))
    grad_part = 0.0
    for d_rows, weights in ((cut(d_all, k * few, few, 1), w_part), (d_other, w_other)):
        grad_part = grad_part + lax.dot_general(
            d_rows.reshape(nz * few, columns),
            weights.reshape(ny * rows, columns),
            contract_cols,
            preferred_element_type=f32,
        )
    grad_part = grad_part.astype(bf16)
    grad_part, over_k = lax.optimization_barrier((grad_part, over_k))
    arrived = [
        shifted(cut(grad_part, lax.rem(y - x - u + 2 * ny, ny) * rows, rows, 1), "x", u)
        for u in range(nx)
    ]

    weight_scale = 1.0 / math.sqrt(tokens)
    contract_rows = (((0,), (0,)), ((), ()))
    d_shares = d_all.reshape(nz, nx, nk, share, columns)
    tile_partial = 0.0
    for core, theirs in ((k, over_x), (1 - k, over_k)):
        d_core = cut(d_shares, core, 1, 2)[:, :, 0]
        d_core = cut(jnp.concatenate([d_core, d_core], axis=1), x, nx, 1)
        tile_partial = tile_partial + lax.dot_general(
            theirs.reshape(-1, ny * rows),
            d_core.reshape(-1, columns),
            contract_rows,
            preferred_element_type=f32,
        )
    tile_partial = (tile_partial * weight_scale).astype(bf16).reshape(ny, rows, columns)
    pieces = [shifted(tile_partial[r], "y", r) for r in range(ny)]
    placed = sum(a.astype(f32) for a in arrived).astype(bf16).reshape(nz, few, rows)
    placed, pieces = lax.optimization_barrier((placed, pieces))
    tile = sum(a.astype(f32) for a in pieces).astype(bf16)
    grad_wq = tile[:, :query_cols]
    grad_wkv = tile[:, query_cols:]
    tile_f = tile.astype(f32)
    tile_square = jnp.sum(tile_f * tile_f)

    row = y * nz + z
    gain_row = cut(gain, row * rows, rows, 0)
    gain_scale = 1.0 / (weight_scale * math.sqrt(all_tokens))
    gain_terms = jnp.sum(tile_f * w_tile.astype(f32), axis=1) * gain_scale / gain_row
    lanes = 128
    packed = jnp.concatenate([gain_terms, jnp.broadcast_to(tile_square / lanes, (lanes,))])
    packed = added(added(packed.reshape(-1, lanes), "k"), "x")
    split = rows // lanes
    packed = copies(packed, ROW)

    placed = rolled(placed, z)
    placed = lax.all_to_all(placed, "z", 0, 0, tiled=True)
    placed = jnp.moveaxis(placed, 0, 1).reshape(few, part)
    their_input = cut(cut(layer_input, k * few, few, 0), x * part, part, 1).astype(f32)
    dots = jnp.sum(placed.astype(f32) * their_input * cut(gain, x * part, part, 0), axis=1)
    dots = added(dots, "x")

    def by_half(own, other):
        return jnp.concatenate(
            [jnp.where(k == 0, own, other), jnp.where(k == 0, other, own)], axis=0
        )

    token_dot = by_half(dots, shifted(dots, "k", 1))[:, None]
    own_grad = cut(placed, k * half, half, 1)
    other_grad = shifted(cut(placed, (1 - k) * half, half, 1), "k", 1)
    feature_grad = by_half(own_grad, other_grad).astype(f32)

    inputs = layer_input.astype(f32)
    inv_rms = lax.rsqrt(jnp.mean(inputs * inputs, axis=1, keepdims=True) + epsilon)
    input_part = cut(layer_input, col * half, half, 1).astype(f32)
    weighted = cut(gain, col * half, half, 0) * feature_grad
    d_input = (
        d_resid.astype(f32)
        + inv_rms * weighted
        - input_part * inv_rms**3 * token_dot / width
    ).astype(bf16)

    is_square = lax.broadcasted_iota(jnp.int32, packed.shape, 1) == split
    grand_total = jnp.sum(jnp.where(is_square, packed, packed * packed))
    grad_square_sum = grand_total / f32(width)
    per_col = ny * nz // (nx * nk)
    grad_gain = cut(packed, col * per_col, per_col, 0)[:, :split].reshape(half)
    return (d_input, grad_wq, grad_wkv, grad_gain, grad_square_sum)


def solution(mesh):
    torus = Mesh(mesh.devices.reshape(4, 8, 4, 2), ("y", "z", "x", "k"))
    both = P(ROW, COL)
    in_specs = (P(ROW, None), P(), both, both, both, both, both)
    out_specs = (both, both, both, P(COL), P())
    return jax.shard_map(local, mesh=torus, in_specs=in_specs, out_specs=out_specs, check_vma=False)
```

```python
import math

import jax
import jax.numpy as jnp
from jax import lax
from jax.sharding import Mesh
from jax.sharding import PartitionSpec as P


ROW = ("y", "z")
COL = ("x", "k")
CHUNKS = 1
f32 = jnp.float32
bf16 = jnp.bfloat16

epsilon = 1e-05


def shifted(block, axis, step):
    count = lax.axis_size(axis)
    if step % count == 0:
        return block
    ring = [(i, (i + step) % count) for i in range(count)]
    return lax.ppermute(block, axis, ring)


def added(block, axis):
    count = lax.axis_size(axis)
    return sum(shifted(block, axis, s) for s in range(1, count)) + block


def copies(block, axis):
    count = lax.axis_size(axis)
    spread = jnp.broadcast_to(block[None], (count, *block.shape))
    return lax.all_to_all(spread, axis, 0, 0, tiled=True)


def cut(array, at, size, axis):
    return lax.dynamic_slice_in_dim(array, at, size, axis)


def local(layer_input, gain, d_query, d_keyval, w_query, w_keyval, d_resid):
    ny, nz, nx, nk = (lax.axis_size(a) for a in ("y", "z", "x", "k"))
    y, z, x, k = (lax.axis_index(a) for a in ("y", "z", "x", "k"))
    tokens, width = layer_input.shape
    all_tokens = tokens * ny * nz
    part = width // ny
    half = part // nk
    rows = part // nz
    query_cols = d_query.shape[1]
    col = x * nk + k

    w_tile = jnp.concatenate([w_query, w_keyval], axis=1)
    w_tile, layer_input = lax.optimization_barrier((w_tile, layer_input))
    w_part = lax.all_gather(w_tile, "z", axis=0, tiled=True)

    share = tokens // (nx * nk)
    mine = cut(layer_input, col * share, share, 0).astype(f32)
    scale = lax.rsqrt(jnp.mean(mine * mine, axis=1, keepdims=True) + epsilon)
    normed = (mine * scale * gain).astype(bf16)
    over_y = [
        shifted(cut(normed, lax.rem(y + s, ny) * part, part, 1), "y", s)
        for s in range(1, ny)
    ]
    over_y = jnp.stack(over_y)

    d_tile = jnp.concatenate([d_query, d_keyval], axis=1)
    columns = d_tile.shape[1]
    d_part = jnp.stack([shifted(d_tile, "y", s) for s in range(ny)])

    over_x = jnp.stack([shifted(over_y, "x", -s) for s in range(nx)], axis=1)
    over_x, d_part = lax.optimization_barrier((over_x, d_part))
    over_k = shifted(over_x, "k", 1)

    inputs = layer_input.astype(f32)
    inv_rms = lax.rsqrt(jnp.mean(inputs * inputs, axis=1, keepdims=True) + epsilon)
    own_input = cut(layer_input, y * part, part, 1).astype(f32)
    own_normed = (own_input * inv_rms * cut(gain, y * part, part, 0)).astype(bf16)

    weight_scale = 1.0 / math.sqrt(tokens)
    contract_rows = (((0,), (0,)), ((), ()))
    tile_partial = lax.dot_general(
        own_normed, d_tile, contract_rows, preferred_element_type=f32
    )
    d_shares = d_part[1:].reshape(ny - 1, nx, nk, share, columns)
    for core, theirs in ((k, over_x), (1 - k, over_k)):
        d_core = cut(d_shares, core, 1, 2)[:, :, 0]
        d_core = cut(jnp.concatenate([d_core, d_core], axis=1), x, nx, 1)
        tile_partial = tile_partial + lax.dot_general(
            theirs.reshape(-1, part),
            d_core.reshape(-1, columns),
            contract_rows,
            preferred_element_type=f32,
        )
    tile_partial = (tile_partial * weight_scale).astype(bf16)
    tile = lax.psum_scatter(tile_partial, "z", scatter_dimension=0, tiled=True)
    grad_wq = tile[:, :query_cols]
    grad_wkv = tile[:, query_cols:]
    tile_f = tile.astype(f32)
    tile_square = jnp.sum(tile_f * tile_f)

    contract_cols = (((1,), (1,)), ((), ()))
    w_other = cut(w_part, (1 - k) * half, half, 0)
    w_own = cut(w_part, k * half, half, 0)
    step = tokens // CHUNKS
    placed, homes = [], []
    for c in range(CHUNKS):
        d_rows = d_part[:, c * step : (c + 1) * step].reshape(ny * step, columns)
        other = lax.dot_general(d_rows, w_other, contract_cols, preferred_element_type=f32)
        other = shifted(other.astype(bf16), "k", 1)
        own = lax.dot_general(d_rows, w_own, contract_cols, preferred_element_type=f32)
        both = (own + other.astype(f32)).astype(bf16).reshape(ny, step, half)
        home = jnp.stack([shifted(both[s], "y", -s) for s in range(ny)])
        homes.append(home)
        sent = [
            lax.dynamic_index_in_dim(home, lax.rem(x + s - y + ny, ny), 0, False)
            for s in range(nx)
        ]
        arrived = [shifted(sent[s], "x", s) for s in range(nx)]
        placed.append(arrived)
    dots = 0.0
    for s in range(ny):
        at = lax.rem(y + s, ny) * part + k * half
        piece = jnp.concatenate([home[s] for home in homes], axis=0).astype(f32)
        their_input = cut(layer_input, at, half, 1).astype(f32)
        dots = dots + jnp.sum(piece * their_input * cut(gain, at, half, 0), axis=1)

    row = y * nz + z
    gain_row = cut(gain, row * rows, rows, 0)
    gain_scale = 1.0 / (weight_scale * math.sqrt(all_tokens))
    gain_terms = jnp.sum(tile_f * w_tile.astype(f32), axis=1) * gain_scale / gain_row

    lanes = 128
    packed = jnp.concatenate([gain_terms, jnp.broadcast_to(tile_square / lanes, (lanes,)), dots])
    packed = added(packed.reshape(-1, lanes), "k")
    packed = added(packed, "x")
    placed[-1], _ = lax.optimization_barrier((placed[-1], packed))
    split = rows // lanes + 1
    token_dot = packed[split:].reshape(tokens, 1)
    packed = copies(packed[:split], ROW)
    feature_grad = jnp.concatenate(
        [sum(a.astype(f32) for a in arrived) for arrived in placed], axis=0
    )

    input_part = cut(layer_input, col * half, half, 1).astype(f32)
    gain_part = cut(gain, col * half, half, 0)
    weighted = gain_part * feature_grad
    d_input = (
        d_resid.astype(f32)
        + inv_rms * weighted
        - input_part * inv_rms**3 * token_dot / width
    ).astype(bf16)

    is_square = lax.broadcasted_iota(jnp.int32, packed.shape, 1) == split - 1
    grand_total = jnp.sum(jnp.where(is_square, packed, packed * packed))
    grad_square_sum = grand_total / f32(width)
    per_col = ny * nz // (nx * nk)
    grad_gain = cut(packed, col * per_col, per_col, 0)[:, : split - 1].reshape(half)
    return (d_input, grad_wq, grad_wkv, grad_gain, grad_square_sum)


def solution(mesh):
    torus = Mesh(mesh.devices.reshape(4, 8, 4, 2), ("y", "z", "x", "k"))
    both = P(ROW, COL)
    in_specs = (P(ROW, None), P(), both, both, both, both, both)
    out_specs = (both, both, both, P(COL), P())
    return jax.shard_map(local, mesh=torus, in_specs=in_specs, out_specs=out_specs, check_vma=False)
```

```python
import math

import jax
import jax.numpy as jnp
from jax import lax
from jax.sharding import Mesh
from jax.sharding import PartitionSpec as P


ROW = ("y", "z")
COL = ("x", "k")
CHUNKS = 2
f32 = jnp.float32
bf16 = jnp.bfloat16

epsilon = 1e-05


def shifted(block, axis, step):
    count = lax.axis_size(axis)
    if step % count == 0:
        return block
    ring = [(i, (i + step) % count) for i in range(count)]
    return lax.ppermute(block, axis, ring)


def copies(block, axis):
    count = lax.axis_size(axis)
    spread = jnp.broadcast_to(block[None], (count, *block.shape))
    return lax.all_to_all(spread, axis, 0, 0, tiled=True)


def cut(array, at, size, axis):
    return lax.dynamic_slice_in_dim(array, at, size, axis)


def local(layer_input, gain, d_query, d_keyval, w_query, w_keyval, d_resid):
    ny, nz, nx, nk = (lax.axis_size(a) for a in ("y", "z", "x", "k"))
    y, z, x, k = (lax.axis_index(a) for a in ("y", "z", "x", "k"))
    tokens, width = layer_input.shape
    all_tokens = tokens * ny * nz
    part = width // ny
    half = part // nk
    rows = part // nz
    query_cols = d_query.shape[1]
    col = x * nk + k

    w_tile = jnp.concatenate([w_query, w_keyval], axis=1)
    w_tile, layer_input = lax.optimization_barrier((w_tile, layer_input))
    w_part = lax.all_gather(w_tile, "z", axis=0, tiled=True)

    share = tokens // (nx * nk)
    mine = cut(layer_input, col * share, share, 0).astype(f32)
    scale = lax.rsqrt(jnp.mean(mine * mine, axis=1, keepdims=True) + epsilon)
    normed = (mine * scale * gain).astype(bf16)
    over_y = [
        shifted(cut(normed, lax.rem(y + s, ny) * part, part, 1), "y", s)
        for s in range(1, ny)
    ]
    over_y = jnp.stack(over_y)

    d_tile = jnp.concatenate([d_query, d_keyval], axis=1)
    columns = d_tile.shape[1]
    d_part = jnp.stack([shifted(d_tile, "y", s) for s in range(ny)])

    over_x = jnp.stack([shifted(over_y, "x", -s) for s in range(nx)], axis=1)
    over_x, d_part = lax.optimization_barrier((over_x, d_part))
    over_k = shifted(over_x, "k", 1)

    inputs = layer_input.astype(f32)
    inv_rms = lax.rsqrt(jnp.mean(inputs * inputs, axis=1, keepdims=True) + epsilon)
    own_input = cut(layer_input, y * part, part, 1).astype(f32)
    own_normed = (own_input * inv_rms * cut(gain, y * part, part, 0)).astype(bf16)

    weight_scale = 1.0 / math.sqrt(tokens)
    contract_rows = (((0,), (0,)), ((), ()))
    tile_partial = lax.dot_general(
        own_normed, d_tile, contract_rows, preferred_element_type=f32
    )
    d_shares = d_part[1:].reshape(ny - 1, nx, nk, share, columns)
    for core, theirs in ((k, over_x), (1 - k, over_k)):
        d_core = cut(d_shares, core, 1, 2)[:, :, 0]
        d_core = cut(jnp.concatenate([d_core, d_core], axis=1), x, nx, 1)
        tile_partial = tile_partial + lax.dot_general(
            theirs.reshape(-1, part),
            d_core.reshape(-1, columns),
            contract_rows,
            preferred_element_type=f32,
        )
    tile_partial = (tile_partial * weight_scale).astype(bf16)
    tile = lax.psum_scatter(tile_partial, "z", scatter_dimension=0, tiled=True)
    grad_wq = tile[:, :query_cols]
    grad_wkv = tile[:, query_cols:]
    tile_f = tile.astype(f32)
    tile_square = jnp.sum(tile_f * tile_f)

    contract_cols = (((1,), (1,)), ((), ()))
    w_other = cut(w_part, (1 - k) * half, half, 0)
    w_own = cut(w_part, k * half, half, 0)
    step = tokens // CHUNKS
    placed, homes = [], []
    for c in range(CHUNKS):
        d_rows = d_part[:, c * step : (c + 1) * step].reshape(ny * step, columns)
        other = lax.dot_general(d_rows, w_other, contract_cols, preferred_element_type=f32)
        other = shifted(other.astype(bf16), "k", 1)
        own = lax.dot_general(d_rows, w_own, contract_cols, preferred_element_type=f32)
        both = (own + other.astype(f32)).astype(bf16).reshape(ny, step, half)
        home = jnp.stack([shifted(both[s], "y", -s) for s in range(ny)])
        homes.append(home)
        sent = [
            lax.dynamic_index_in_dim(home, lax.rem(x + s - y + ny, ny), 0, False)
            for s in range(nx)
        ]
        arrived = [shifted(sent[s], "x", s) for s in range(nx)]
        placed.append(arrived)
    dots = 0.0
    for s in range(ny):
        at = lax.rem(y + s, ny) * part + k * half
        piece = jnp.concatenate([home[s] for home in homes], axis=0).astype(f32)
        their_input = cut(layer_input, at, half, 1).astype(f32)
        dots = dots + jnp.sum(piece * their_input * cut(gain, at, half, 0), axis=1)

    row = y * nz + z
    gain_row = cut(gain, row * rows, rows, 0)
    gain_scale = 1.0 / (weight_scale * math.sqrt(all_tokens))
    gain_terms = jnp.sum(tile_f * w_tile.astype(f32), axis=1) * gain_scale / gain_row

    lanes = 128
    packed = jnp.concatenate([gain_terms, jnp.broadcast_to(tile_square / lanes, (lanes,)), dots])
    split = rows // lanes + 1
    packed = packed.reshape(-1, lanes)
    count = packed.shape[0]
    packed = copies(packed, ("z", "k"))
    packed = packed.reshape(nz, nk, count, lanes)
    packed = jnp.sum(packed, axis=1).reshape(nz * count, lanes)
    placed[-1], _ = lax.optimization_barrier((placed[-1], packed))
    packed = copies(packed, ("y", "x")).reshape(ny, nx, nz * count, lanes)
    packed = jnp.sum(packed, axis=1).reshape(ny * nz, count, lanes)
    token_dot = cut(packed, row, 1, 0)[0, split:].reshape(tokens, 1)
    feature_grad = jnp.concatenate(
        [sum(a.astype(f32) for a in arrived) for arrived in placed], axis=0
    )

    input_part = cut(layer_input, col * half, half, 1).astype(f32)
    gain_part = cut(gain, col * half, half, 0)
    weighted = gain_part * feature_grad
    d_input = (
        d_resid.astype(f32)
        + inv_rms * weighted
        - input_part * inv_rms**3 * token_dot / width
    ).astype(bf16)

    at = lax.broadcasted_iota(jnp.int32, packed.shape, 1)
    terms = jnp.where(at == split - 1, packed, packed * packed)
    grand_total = jnp.sum(jnp.where(at < split, terms, 0.0))
    grad_square_sum = grand_total / f32(width)
    per_col = ny * nz // (nx * nk)
    grad_gain = cut(packed, col * per_col, per_col, 0)[:, : split - 1].reshape(half)
    return (d_input, grad_wq, grad_wkv, grad_gain, grad_square_sum)


def solution(mesh):
    torus = Mesh(mesh.devices.reshape(4, 8, 4, 2), ("y", "z", "x", "k"))
    both = P(ROW, COL)
    in_specs = (P(ROW, None), P(), both, both, both, both, both)
    out_specs = (both, both, both, P(COL), P())
    return jax.shard_map(local, mesh=torus, in_specs=in_specs, out_specs=out_specs, check_vma=False)
```

```python
import math

import jax
import jax.numpy as jnp
from jax import lax
from jax.sharding import Mesh
from jax.sharding import PartitionSpec as P


ROW = ("y", "z")
COL = ("x", "k")
CHUNKS = 2
f32 = jnp.float32
bf16 = jnp.bfloat16

epsilon = 1e-05


def shifted(block, axis, step):
    count = lax.axis_size(axis)
    if step % count == 0:
        return block
    ring = [(i, (i + step) % count) for i in range(count)]
    return lax.ppermute(block, axis, ring)


def copies(block, axis):
    count = lax.axis_size(axis)
    spread = jnp.broadcast_to(block[None], (count, *block.shape))
    return lax.all_to_all(spread, axis, 0, 0, tiled=True)


def cut(array, at, size, axis):
    return lax.dynamic_slice_in_dim(array, at, size, axis)


def local(layer_input, gain, d_query, d_keyval, w_query, w_keyval, d_resid):
    ny, nz, nx, nk = (lax.axis_size(a) for a in ("y", "z", "x", "k"))
    y, z, x, k = (lax.axis_index(a) for a in ("y", "z", "x", "k"))
    tokens, width = layer_input.shape
    all_tokens = tokens * ny * nz
    part = width // ny
    half = part // nk
    rows = part // nz
    query_cols = d_query.shape[1]
    col = x * nk + k

    w_tile = jnp.concatenate([w_query, w_keyval], axis=1)
    w_tile, layer_input = lax.optimization_barrier((w_tile, layer_input))
    w_part = lax.all_gather(w_tile, "z", axis=0, tiled=True)

    share = tokens // (nx * nk)
    mine = cut(layer_input, col * share, share, 0).astype(f32)
    scale = lax.rsqrt(jnp.mean(mine * mine, axis=1, keepdims=True) + epsilon)
    normed = (mine * scale * gain).astype(bf16)
    over_y = [
        shifted(cut(normed, lax.rem(y + s, ny) * part, part, 1), "y", s)
        for s in range(1, ny)
    ]
    over_y = jnp.stack(over_y)

    d_tile = jnp.concatenate([d_query, d_keyval], axis=1)
    columns = d_tile.shape[1]
    d_part = jnp.stack([shifted(d_tile, "y", s) for s in range(ny)])

    over_x = jnp.stack([shifted(over_y, "x", -s) for s in range(nx)], axis=1)
    over_x, d_part = lax.optimization_barrier((over_x, d_part))
    over_k = shifted(over_x, "k", 1)

    inputs = layer_input.astype(f32)
    inv_rms = lax.rsqrt(jnp.mean(inputs * inputs, axis=1, keepdims=True) + epsilon)
    own_input = cut(layer_input, y * part, part, 1).astype(f32)
    own_normed = (own_input * inv_rms * cut(gain, y * part, part, 0)).astype(bf16)

    weight_scale = 1.0 / math.sqrt(tokens)
    contract_rows = (((0,), (0,)), ((), ()))
    tile_partial = lax.dot_general(
        own_normed, d_tile, contract_rows, preferred_element_type=f32
    )
    d_shares = d_part[1:].reshape(ny - 1, nx, nk, share, columns)
    for core, theirs in ((k, over_x), (1 - k, over_k)):
        d_core = cut(d_shares, core, 1, 2)[:, :, 0]
        d_core = cut(jnp.concatenate([d_core, d_core], axis=1), x, nx, 1)
        tile_partial = tile_partial + lax.dot_general(
            theirs.reshape(-1, part),
            d_core.reshape(-1, columns),
            contract_rows,
            preferred_element_type=f32,
        )
    tile_partial = (tile_partial * weight_scale).astype(bf16)
    tile = lax.psum_scatter(tile_partial, "z", scatter_dimension=0, tiled=True)
    grad_wq = tile[:, :query_cols]
    grad_wkv = tile[:, query_cols:]
    tile_f = tile.astype(f32)
    tile_square = jnp.sum(tile_f * tile_f)

    contract_cols = (((1,), (1,)), ((), ()))
    w_other = cut(w_part, (1 - k) * half, half, 0)
    w_own = cut(w_part, k * half, half, 0)
    step = tokens // CHUNKS
    placed, homes = [], []
    for c in range(CHUNKS):
        d_rows = d_part[:, c * step : (c + 1) * step].reshape(ny * step, columns)
        other = lax.dot_general(d_rows, w_other, contract_cols, preferred_element_type=f32)
        other = shifted(other.astype(bf16), "k", 1)
        own = lax.dot_general(d_rows, w_own, contract_cols, preferred_element_type=f32)
        both = (own + other.astype(f32)).astype(bf16).reshape(ny, step, half)
        home = jnp.stack([shifted(both[s], "y", -s) for s in range(ny)])
        homes.append(home)
        sent = [
            lax.dynamic_index_in_dim(home, lax.rem(x + s - y + ny, ny), 0, False)
            for s in range(nx)
        ]
        arrived = [shifted(sent[s], "x", s) for s in range(nx)]
        placed.append(arrived)
    dots = 0.0
    for s in range(ny):
        at = lax.rem(y + s, ny) * part + k * half
        piece = jnp.concatenate([home[s] for home in homes], axis=0).astype(f32)
        their_input = cut(layer_input, at, half, 1).astype(f32)
        dots = dots + jnp.sum(piece * their_input * cut(gain, at, half, 0), axis=1)

    row = y * nz + z
    gain_row = cut(gain, row * rows, rows, 0)
    gain_scale = 1.0 / (weight_scale * math.sqrt(all_tokens))
    gain_terms = jnp.sum(tile_f * w_tile.astype(f32), axis=1) * gain_scale / gain_row

    lanes = 128
    packed = jnp.concatenate([gain_terms, jnp.broadcast_to(tile_square / lanes, (lanes,)), dots])
    packed = copies(packed.reshape(-1, lanes), COL)
    packed = jnp.sum(packed, axis=0)
    placed[-1], _ = lax.optimization_barrier((placed[-1], packed))
    split = rows // lanes + 1
    token_dot = packed[split:].reshape(tokens, 1)
    packed = copies(packed[:split], ROW)
    feature_grad = jnp.concatenate(
        [sum(a.astype(f32) for a in arrived) for arrived in placed], axis=0
    )

    input_part = cut(layer_input, col * half, half, 1).astype(f32)
    gain_part = cut(gain, col * half, half, 0)
    weighted = gain_part * feature_grad
    d_input = (
        d_resid.astype(f32)
        + inv_rms * weighted
        - input_part * inv_rms**3 * token_dot / width
    ).astype(bf16)

    is_square = lax.broadcasted_iota(jnp.int32, packed.shape, 1) == split - 1
    grand_total = jnp.sum(jnp.where(is_square, packed, packed * packed))
    grad_square_sum = grand_total / f32(width)
    per_col = ny * nz // (nx * nk)
    grad_gain = cut(packed, col * per_col, per_col, 0)[:, : split - 1].reshape(half)
    return (d_input, grad_wq, grad_wkv, grad_gain, grad_square_sum)


def solution(mesh):
    torus = Mesh(mesh.devices.reshape(4, 8, 4, 2), ("y", "z", "x", "k"))
    both = P(ROW, COL)
    in_specs = (P(ROW, None), P(), both, both, both, both, both)
    out_specs = (both, both, both, P(COL), P())
    return jax.shard_map(local, mesh=torus, in_specs=in_specs, out_specs=out_specs, check_vma=False)
```
